1024 devices in a mesh: band: 16 (over z), patch: 64 (over x, y, core).
Axes of the slice: x: 4, y: 8, z: 16, core: 2. Of those that a mesh axis runs over, the one named last changes fastest.
Arguments:
- grid_feat: bfloat16 [262144, 474], P(('band', 'patch')), may hold values from -6 to 6
- enc_sender: int32 [393216], P(('band', 'patch')), may hold values from 0 to 255
- enc_patch: int32 [393216, 1], P(('band', 'patch')), may hold values from 0 to 63; in each aligned block of 384 rows (0 to 383, 384 to 767, ...) at most 8 rows name the same one
- enc_node: int32 [393216], P(('band', 'patch')), may hold values from 0 to 319
- enc_geo: bfloat16 [4, 393216], P(None, ('band', 'patch')), may hold values from -6 to 6
- mesh_nodes: bfloat16 [20480, 512], P('patch'), may hold values from -6 to 6
- mesh_edge: bfloat16 [262144, 512], P(('band', 'patch')), may hold values from -6 to 6
- mesh_send: int32 [262144], P(('band', 'patch')), may hold values from 0 to 575
- mesh_recv: int32 [262144], P(('band', 'patch')), may hold values from 0 to 319
- halo_rows: int32 [64, 256], P('patch'), may hold values from 0 to 319
- grid_in: bfloat16 [474, 512], replicated, may hold values from -0.25 to 0.25
- grid_out: bfloat16 [512, 512], replicated, may hold values from -0.25 to 0.25
- geo_weight: bfloat16 [4, 512], replicated, may hold values from -3 to 3
- enc_edge_w: bfloat16 [3, 512, 512], replicated, may hold values from -0.25 to 0.25
- enc_node_w: bfloat16 [3, 512, 512], replicated, may hold values from -0.25 to 0.25
- proc_edge_w: bfloat16 [4, 512, 512], replicated, may hold values from -0.25 to 0.25
- proc_node_w: bfloat16 [3, 512, 512], replicated, may hold values from -0.25 to 0.25
Outputs:
- mesh_two: bfloat16 [20480, 512], P('patch')
- edge_out: bfloat16 [262144, 512], P(('band', 'patch'))
The draws below stay inside these ranges and needn't reach their ends.
Inputs may be any that keep to these rules, and one draw needn't show every extreme that they name: `enc_sender`: row among the 256 grid rows of the device that holds the edge. `enc_patch`: among the 384 edge rows of one device no patch is named more than 8 times; some patch exactly 8 times. `mesh_send`: values from 320 on name rows received from other patches, as in the reference program. `halo_rows`: row q holds, in blocks of 4, the rows of patch q sent to patches 0, 1, ...
All inputs are finite; a program needn't handle non-finite values.
Results may differ from the reference program's by a relative error of at most 0.017.
Values may be sent and summed in bfloat16 or wider, within the bound.
A program may use at most 32 MiB of HBM per device.

```python
import math
import jax
import jax.numpy as jnp
import numpy as np
from jax import lax

D = 512
C_IN = 474
G_DEV = 256
E_DEV = 384
M_DEV = 320
ME_DEV = 256
HALO_DEV = 256
CAP = 8
H_PEER = 4
GRID = 262144
EDGES = 393216
MESH = 20480
MEDGES = 262144
N_BAND = 16
N_PATCH = 64


def touch_ends(drawn, key, smallest, high):
    longest = drawn.shape.index(max(drawn.shape))
    spots = []
    for shift in (0, 1):
        where = [jax.random.randint(jax.random.fold_in(key, axis), (), 0, length) for axis, length in enumerate(drawn.shape)]
        where[longest] = (where[longest] + shift) % drawn.shape[longest]
        spots.append(tuple(where))
    return drawn.at[spots[0]].set(smallest).at[spots[1]].set(high)


def block_scale(own_key, dims, split, least, largest):
    level = 1.0
    for position, blocks in split:
        draws = jax.random.uniform(jax.random.fold_in(jax.random.fold_in(own_key, 6), position), (blocks,), jnp.float32, least / len(split), largest / len(split))
        level = level * jnp.repeat(jnp.exp(draws), dims[position] // blocks).reshape((-1,) + (1,) * (len(dims) - 1 - position))
    return level


def shared_out(rng, own, number, rows, count, top, limit, skew):
    ranking = jax.random.permutation(rng, count)
    crowded, common = shares(count, rows * top, limit, skew, True), shares(count, rows * top, limit, skew, False)
    places = jnp.arange(count)

    def named(lengths, turn):
        used = int((lengths > 0).sum())
        fixed = max(1, used // 4)
        passed = fixed + (places - fixed + turn * (used - fixed)) % max(1, count - fixed)
        return jnp.zeros((count,), jnp.int32).at[ranking[jnp.where(places < fixed, places, passed)]].set(jnp.asarray(lengths, jnp.int32))

    lengths = jnp.where(number % 4 == 0, named(crowded, number // 4), named(common, number - number // 4 - 1))
    mixed = jax.random.permutation(jax.random.fold_in(own, 3), count)
    donor, taker = mixed[0:count // 2 * 2:2], mixed[1:count // 2 * 2:2]
    slack = jnp.minimum(lengths[donor] - 1, limit - lengths[taker]) // 2
    slack = jnp.where((donor == ranking[0]) | (taker == ranking[0]) | (lengths[taker] == 0), 0, jnp.maximum(slack, 0))
    passed = jax.random.randint(jax.random.fold_in(own, 4), (count // 2,), 0, 1 << 20) % (slack + 1)
    lengths = lengths.at[donor].add(-passed).at[taker].add(passed)
    items = jnp.searchsorted(jnp.cumsum(lengths), jnp.arange(rows * top), side="right").astype(jnp.int32)
    table = items.reshape(top, rows).T
    table = table[jax.random.permutation(jax.random.fold_in(own, 1), rows)]
    turn = jax.random.randint(jax.random.fold_in(own, 2), (rows, 1), 0, top)
    return jnp.take_along_axis(table, (jnp.arange(top)[None, :] + turn) % top, axis=1)


def shares(count, total, bound, skew, full):
    weights = [(1 << 20) // math.isqrt(standing ** skew) + 1 for standing in range(1, count + 1)]
    largest = bound if full else min(bound, max(-(-total // count), total * weights[0] // sum(weights)))
    least = 1 if total - largest >= count - 1 else 0
    holding, spare = [largest] + [least] * (count - 1), total - largest - least * (count - 1)
    while spare > 0:
        candidates = [i for i in range(1, count) if holding[i] < largest] or [i for i in range(1, count) if holding[i] < bound]
        mass, budget = sum([weights[i] for i in candidates]), spare
        for i in candidates:
            addition = min(bound - holding[i], max(1, budget * weights[i] // mass), spare)
            holding[i] = holding[i] + addition
            spare = spare - addition
    return np.array(holding)


def scatter_about(rng, dims, width, limit, cuts=(), kind=jnp.bfloat16):
    gain = block_scale(rng, dims, cuts, -0.22, 0.18) if cuts else 1.0
    drawn = jax.random.normal(rng, dims, jnp.float32) * width * gain
    return jnp.minimum(jnp.maximum(drawn, -limit), limit).astype(kind)


def setup_inputs(seed: int = 0) -> dict:
    splits = jax.random.split(jax.random.key(seed), 18)
    grid_feat = scatter_about(splits[0], (GRID, C_IN), 1.0, 6.0, ((0, 1024),))
    enc_sender = touch_ends(jax.random.randint(splits[1], (EDGES,), 0, G_DEV), jax.random.fold_in(splits[1], 1), 0, G_DEV - 1).astype(jnp.int32)
    enc_patch_keys = jax.random.split(jax.random.fold_in(splits[2], 1), EDGES // E_DEV)
    enc_patch_turns = jax.random.permutation(jax.random.fold_in(splits[2], 3), EDGES // E_DEV)
    enc_patch = jax.vmap(lambda own, number: shared_out(jax.random.fold_in(splits[2], 2), own, number, E_DEV, N_PATCH, 1, CAP, 1))(enc_patch_keys, enc_patch_turns).reshape((EDGES, 1))
    enc_node = touch_ends(jax.random.randint(splits[3], (EDGES,), 0, M_DEV), jax.random.fold_in(splits[3], 1), 0, M_DEV - 1).astype(jnp.int32)
    enc_geo = scatter_about(splits[4], (4, EDGES), 1.0, 6.0, ((1, 1024),))
    mesh_nodes = scatter_about(splits[5], (MESH, D), 1.0, 6.0, ((0, 64),))
    mesh_edge = scatter_about(splits[6], (MEDGES, D), 1.0, 6.0, ((0, 1024),))
    mesh_send = touch_ends(jax.random.randint(splits[7], (MEDGES,), 0, M_DEV + HALO_DEV), jax.random.fold_in(splits[7], 1), 0, (M_DEV + HALO_DEV) - 1).astype(jnp.int32)
    mesh_recv = touch_ends(jax.random.randint(splits[8], (MEDGES,), 0, M_DEV), jax.random.fold_in(splits[8], 1), 0, M_DEV - 1).astype(jnp.int32)
    halo_rows = touch_ends(jax.random.randint(splits[9], (N_PATCH, HALO_DEV), 0, M_DEV), jax.random.fold_in(splits[9], 1), 0, M_DEV - 1).astype(jnp.int32)
    grid_in = scatter_about(splits[10], (C_IN, D), C_IN ** -0.5, 0.25)
    grid_out = scatter_about(splits[11], (D, D), D ** -0.5, 0.25)
    geo_weight = scatter_about(splits[12], (4, D), 4 ** -0.5, 3.0)
    enc_edge_w = scatter_about(splits[13], (3, D, D), D ** -0.5, 0.25)
    enc_node_w = scatter_about(splits[14], (3, D, D), D ** -0.5, 0.25)
    proc_edge_w = scatter_about(splits[15], (4, D, D), D ** -0.5, 0.25)
    proc_node_w = scatter_about(splits[16], (3, D, D), D ** -0.5, 0.25)
    return {"grid_feat": grid_feat, "enc_sender": enc_sender, "enc_patch": enc_patch, "enc_node": enc_node, "enc_geo": enc_geo, "mesh_nodes": mesh_nodes, "mesh_edge": mesh_edge, "mesh_send": mesh_send, "mesh_recv": mesh_recv, "halo_rows": halo_rows, "grid_in": grid_in, "grid_out": grid_out, "geo_weight": geo_weight, "enc_edge_w": enc_edge_w, "enc_node_w": enc_node_w, "proc_edge_w": proc_edge_w, "proc_node_w": proc_node_w}


def norm_rows(values_in):
    average = lax.optimization_barrier(jnp.mean(values_in, axis=-1, keepdims=True))
    centred = values_in - average
    spread = lax.optimization_barrier(jnp.mean(centred * centred, axis=-1, keepdims=True))
    return centred * lax.rsqrt(spread + 1e-05)

def network_tail(preact, out_weight):
    hidden = jax.nn.silu(preact).astype(jnp.bfloat16)
    return norm_rows(jnp.dot(hidden, out_weight, preferred_element_type=jnp.float32))

def update_rows(node_rows, running, weights):
    preact = jnp.dot(node_rows, weights[0], preferred_element_type=jnp.float32) + jnp.dot(running.astype(jnp.bfloat16), weights[1], preferred_element_type=jnp.float32)
    return (node_rows.astype(jnp.float32) + network_tail(preact, weights[2])).astype(jnp.bfloat16)

def reference(grid_feat, enc_sender, enc_patch, enc_node, enc_geo, mesh_nodes, mesh_edge, mesh_send, mesh_recv, halo_rows, grid_in, grid_out, geo_weight, enc_edge_w, enc_node_w, proc_edge_w, proc_node_w):

    def embed_grid(pieces):
        hidden = jax.nn.silu(jnp.dot(pieces, grid_in, preferred_element_type=jnp.float32)).astype(jnp.bfloat16)
        latent = norm_rows(jnp.dot(hidden, grid_out, preferred_element_type=jnp.float32)).astype(jnp.bfloat16)
        return jnp.dot(latent, enc_edge_w[0], preferred_element_type=jnp.float32)
    sender_proj = lax.map(embed_grid, grid_feat.reshape(N_BAND, -1, C_IN)).reshape(GRID, D)
    edge_ids = jnp.arange(EDGES, dtype=jnp.int32)
    senders = enc_sender.astype(jnp.int32) + edge_ids // E_DEV * G_DEV
    receivers = enc_patch[:, 0].astype(jnp.int32) * M_DEV + enc_node.astype(jnp.int32)
    recv_proj = jnp.dot(mesh_nodes, enc_edge_w[1], preferred_element_type=jnp.float32)
    geo_blocks = enc_geo.reshape(4, N_BAND, -1).transpose(1, 0, 2)

    def encode_band(running, pieces):
        send_rows, geo_block, recv_rows = pieces
        geo_term = lax.dot_general(geo_block, geo_weight, (((0,), (0,)), ((), ())), preferred_element_type=jnp.float32)
        send_term = (sender_proj[send_rows] + geo_term).astype(jnp.bfloat16)
        preact = send_term.astype(jnp.float32) + recv_proj[recv_rows]
        message = network_tail(preact, enc_edge_w[2])
        return (running + jax.ops.segment_sum(message, recv_rows, num_segments=MESH), None)
    enc_agg, _ = lax.scan(encode_band, jnp.zeros((MESH, D), jnp.float32), (senders.reshape(N_BAND, -1), geo_blocks, receivers.reshape(N_BAND, -1)))
    mesh_one = update_rows(mesh_nodes, enc_agg, enc_node_w)
    sent_proj = jnp.dot(mesh_one, proc_edge_w[1], preferred_element_type=jnp.float32).astype(jnp.bfloat16)
    recv_two = jnp.dot(mesh_one, proc_edge_w[2], preferred_element_type=jnp.float32)
    mesh_ids = jnp.arange(MEDGES, dtype=jnp.int32)
    patch_of = mesh_ids // ME_DEV % N_PATCH
    sender_local = mesh_send.astype(jnp.int32)
    ghost_index = jnp.maximum(sender_local - M_DEV, 0)
    source = ghost_index // H_PEER
    within = ghost_index % H_PEER
    far_rows = halo_rows.reshape(-1).astype(jnp.int32)[source * HALO_DEV + patch_of * H_PEER + within]
    node_index = jnp.where(sender_local < M_DEV, patch_of * M_DEV + sender_local, source * M_DEV + far_rows)
    target = patch_of * M_DEV + mesh_recv.astype(jnp.int32)

    def process_band(running, pieces):
        edge_block, node_block, target_block = pieces
        preact = jnp.dot(edge_block, proc_edge_w[0], preferred_element_type=jnp.float32) + sent_proj[node_block].astype(jnp.float32) + recv_two[target_block]
        updated = edge_block.astype(jnp.float32) + network_tail(preact, proc_edge_w[3])
        return (running + jax.ops.segment_sum(updated, target_block, num_segments=MESH), updated.astype(jnp.bfloat16))
    proc_agg, edge_blocks = lax.scan(process_band, jnp.zeros((MESH, D), jnp.float32), (mesh_edge.reshape(N_BAND, -1, D), node_index.reshape(N_BAND, -1), target.reshape(N_BAND, -1)))
    mesh_two = update_rows(mesh_one, proc_agg, proc_node_w)
    return (mesh_two, edge_blocks.reshape(MEDGES, D))
```

```python
import jax
import jax.numpy as jnp
from jax import lax
from jax.sharding import Mesh
from jax.sharding import PartitionSpec as P

PATCH = ("patch_0", "patch_1", "patch_2")
BAND_PATCH = ("band", "patch_0", "patch_1", "patch_2")


def cut_along(value, dim, length):
    before, after = (value.shape[:dim], value.shape[dim + 1 :])
    return jnp.moveaxis(value.reshape(*before, length, -1, *after), dim, 0)


def sum_at_owner(value, axis, dim):
    pieces = cut_along(value, dim, lax.axis_size(axis))
    arrived = lax.all_to_all(pieces, axis, split_axis=0, concat_axis=0, tiled=True)
    return arrived.astype(jnp.float32).sum(axis=0)


def laid_out(pieces, dim):
    lengths = list(pieces.shape[1:])
    lengths[dim] *= pieces.shape[0]
    return jnp.moveaxis(pieces, 0, dim).reshape(lengths)


def from_everyone(value, axis):
    length = lax.axis_size(axis)
    return lax.all_to_all(
        jnp.broadcast_to(value[None], (length, *value.shape)), axis, 0, 0, tiled=True
    )


def gather_directly(value, axis, dim):
    return laid_out(from_everyone(value, axis), dim)


def exchange_in_order(pieces, axes, order):
    lengths = [lax.axis_size(a) for a in axes]
    pieces = pieces.reshape(*lengths, *pieces.shape[1:])
    for k in order:
        pieces = lax.all_to_all(pieces, axes[k], split_axis=k, concat_axis=k, tiled=True)
    return pieces.reshape(-1, *pieces.shape[len(axes) :])


def core_and_chips(value, groups, order, split_dim, concat_dim):
    length = lax.axis_size(groups[0]) * lax.axis_size(groups[1])
    pieces = cut_along(value, split_dim, length)
    return laid_out(exchange_in_order(pieces, groups, order), concat_dim)


def norm_rows(values_in):
    average = jnp.mean(values_in, axis=-1, keepdims=True)
    centred = values_in - average
    spread = jnp.mean(centred * centred, axis=-1, keepdims=True)
    return centred * lax.rsqrt(spread + 1e-05)


def network_tail(preact, out_weight):
    hidden = jax.nn.silu(preact).astype(jnp.bfloat16)
    return norm_rows(jnp.dot(hidden, out_weight, preferred_element_type=jnp.float32))


def update_rows(node_rows, running, weights):
    preact = jnp.dot(node_rows, weights[0], preferred_element_type=jnp.float32) + jnp.dot(
        running.astype(jnp.bfloat16), weights[1], preferred_element_type=jnp.float32
    )
    return (node_rows.astype(jnp.float32) + network_tail(preact, weights[2])).astype(jnp.bfloat16)


def node_update(node_rows, partial_value, weights):
    share_rows = sum_at_owner(partial_value.astype(jnp.bfloat16), "band", 0)
    row_count = share_rows.shape[0]
    first_row = lax.axis_index("band") * row_count
    own_rows = lax.dynamic_slice_in_dim(node_rows, first_row, row_count, 0)
    updated = update_rows(own_rows, share_rows, weights)
    return gather_directly(updated, "band", 0)


def per_device(
    grid_feat,
    enc_sender,
    enc_patch,
    enc_node,
    enc_geo,
    mesh_nodes,
    mesh_edge,
    mesh_send,
    mesh_recv,
    halo_rows,
    grid_in,
    grid_out,
    geo_weight,
    enc_edge_w,
    enc_node_w,
    proc_edge_w,
    proc_node_w,
):
    peer_count = lax.axis_size(PATCH)
    latent_width = mesh_nodes.shape[1]
    mesh_count = mesh_nodes.shape[0]
    edge_count = enc_sender.shape[0]
    capacity = 4 * edge_count // (3 * peer_count)
    hidden = jax.nn.silu(jnp.dot(grid_feat, grid_in, preferred_element_type=jnp.float32)).astype(
        jnp.bfloat16
    )
    grid_lat = norm_rows(jnp.dot(hidden, grid_out, preferred_element_type=jnp.float32)).astype(
        jnp.bfloat16
    )
    sender_proj = jnp.dot(grid_lat, enc_edge_w[0], preferred_element_type=jnp.float32)
    geo_term = lax.dot_general(
        enc_geo, geo_weight, (((0,), (0,)), ((), ())), preferred_element_type=jnp.float32
    )
    send_term = (sender_proj[enc_sender] + geo_term).astype(jnp.bfloat16)
    target = enc_patch[:, 0]
    onehot = (target[:, None] == jnp.arange(peer_count, dtype=jnp.int32)[None, :]).astype(jnp.int32)
    slot_index = jnp.sum((jnp.cumsum(onehot, axis=0) - 1) * onehot, axis=1)
    slots = peer_count * capacity
    chosen = (target * capacity + slot_index)[None, :] == jnp.arange(slots, dtype=jnp.int32)[:, None]
    outbox = jnp.dot(
        chosen.astype(jnp.bfloat16), send_term, preferred_element_type=jnp.float32
    ).astype(jnp.bfloat16).reshape(peer_count, capacity, latent_width)
    addresses = jnp.sum(jnp.where(chosen, enc_node[None, :] - mesh_count, 0), axis=1) + mesh_count
    addresses = addresses.reshape(peer_count, capacity)
    recv_proj = jnp.dot(mesh_nodes, enc_edge_w[1], preferred_element_type=jnp.float32)
    sender_terms = core_and_chips(outbox, (("patch_0", "patch_1"), "patch_2"), (1, 0), 0, 0)
    places = core_and_chips(addresses, (("patch_0", "patch_1"), "patch_2"), (1, 0), 0, 0)
    preact = sender_terms.astype(jnp.float32) + recv_proj[jnp.minimum(places, mesh_count - 1)]
    messages, places = (network_tail(preact, enc_edge_w[2]), places)
    landing = jnp.arange(mesh_count, dtype=jnp.int32)[:, None] == places.reshape(-1)[None, :]
    partial_value = jnp.dot(
        landing.astype(jnp.bfloat16),
        messages.reshape(-1, latent_width).astype(jnp.bfloat16),
        preferred_element_type=jnp.float32,
    )
    mesh_one = node_update(mesh_nodes, partial_value, enc_node_w)
    sent_proj = jnp.dot(mesh_one, proc_edge_w[1], preferred_element_type=jnp.float32).astype(
        jnp.bfloat16
    )
    recv_two = jnp.dot(mesh_one, proc_edge_w[2], preferred_element_type=jnp.float32)
    outgoing = sent_proj[halo_rows[0]].reshape(peer_count, -1, latent_width)
    ghosts = lax.all_to_all(outgoing, PATCH, split_axis=0, concat_axis=0, tiled=True)
    lookup = jnp.concatenate([sent_proj, ghosts.reshape(-1, latent_width)], axis=0)
    preact = (
        jnp.dot(mesh_edge, proc_edge_w[0], preferred_element_type=jnp.float32)
        + lookup[mesh_send].astype(jnp.float32)
        + recv_two[mesh_recv]
    )
    edge_new = mesh_edge.astype(jnp.float32) + network_tail(preact, proc_edge_w[3])
    partial_two = jnp.zeros((mesh_count, latent_width), jnp.float32).at[mesh_recv].add(edge_new)
    mesh_two = node_update(mesh_one, partial_two, proc_node_w)
    return (mesh_two, edge_new.astype(jnp.bfloat16))


def solution(mesh):
    split = Mesh(
        mesh.devices.reshape(mesh.shape["band"], 4, 8, 2), ("band", "patch_0", "patch_1", "patch_2")
    )
    placed = (
        P(BAND_PATCH, None),
        P(BAND_PATCH),
        P(BAND_PATCH, None),
        P(BAND_PATCH),
        P(None, BAND_PATCH),
        P(PATCH, None),
        P(BAND_PATCH, None),
        P(BAND_PATCH),
        P(BAND_PATCH),
        P(PATCH, None),
        P(),
        P(),
        P(),
        P(),
        P(),
        P(),
        P(),
    )
    return jax.shard_map(
        per_device,
        mesh=split,
        in_specs=placed,
        out_specs=(P(PATCH, None), P(BAND_PATCH, None)),
        check_vma=False,
    )
```

```python
import functools

import jax
import jax.numpy as jnp
from jax import lax
from jax.experimental import pallas as pl
from jax.experimental.pallas import tpu as pltpu
from jax.sharding import PartitionSpec as P

F32 = jnp.float32
BF16 = jnp.bfloat16
I32 = jnp.int32
MESH = pl.DeviceIdType.MESH
CAP = 8


def mark(condition):
    return jnp.where(condition, 1.0, 0.0).astype(BF16)


def iota(shape, dim):
    return lax.broadcasted_iota(I32, shape, dim)


def mm(a, b):
    return jnp.dot(a, b, preferred_element_type=F32)


def mm_rows(a, b):
    return lax.dot_general(a, b, (((1,), (1,)), ((), ())), preferred_element_type=F32)


def mm_cols(a, b):
    return lax.dot_general(a, b, (((0,), (0,)), ((), ())), preferred_element_type=F32)


def norm_rows(v):
    centred = v - jnp.mean(v, axis=-1, keepdims=True)
    spread = jnp.mean(centred * centred, axis=-1, keepdims=True)
    return centred * lax.rsqrt(spread + 1e-05)


def silu(v):
    return v * jax.nn.sigmoid(v)


def tail(preact, weight):
    return norm_rows(mm(silu(preact).astype(BF16), weight))


def kernel(
    nb, np_, ny,
    gf_h, gi_h, go_h, gw, ee_h, en_h, pe_h, pn_h, mn_h, me_h,
    tgt, snd, nod, geo, msd, mrc, halo,
    two_ref, edge_ref,
    gf, gi, go, ee, en, pe, pn, mn, me, wsem,
    addr_out, addr_in, outbox, inbox, rs_out, rs_in, ag_out, ag_in,
    halo_out, halo_in, rs2_out, rs2_in, ag2_out, ag2_in,
    recv_proj, edge_proj, one_ref, ssem, rsem,
):
    b = lax.axis_index("band")
    p = lax.axis_index("patch")
    edges = tgt.shape[1]
    count, width = mn.shape
    half = width // 2
    share = count // nb
    block = 2 * share
    slots = np_ * CAP
    grid_rows = gf.shape[0]
    medges = me.shape[0]
    padded = -(-share // 16) * 16
    wide = 2 * count

    def peer(i):
        off = (i * 29) % np_
        x = (p // (2 * ny) + off // (2 * ny)) % (np_ // (2 * ny))
        y = (p // 2 + off // 2) % ny
        c = (p + off) % 2
        return x * (2 * ny) + y * 2 + c

    def level(i):
        return (b + i * 7) % nb

    barrier = pltpu.get_barrier_semaphore()

    def greet_patch(i, carry):
        pl.semaphore_signal(barrier, inc=1, device_id={"patch": peer(i)}, device_id_type=MESH)
        return carry

    def greet_band(i, carry):
        pl.semaphore_signal(barrier, inc=1, device_id={"band": level(i)}, device_id_type=MESH)
        return carry

    lax.fori_loop(1, np_, greet_patch, 0)
    lax.fori_loop(1, nb, greet_band, 0)

    loads = [
        pltpu.make_async_copy(src, dst, wsem.at[k])
        for k, (src, dst) in enumerate(
            [(gf_h, gf), (gi_h, gi), (go_h, go), (ee_h, ee), (mn_h, mn), (me_h, me),
             (pe_h, pe), (en_h, en), (pn_h, pn)]
        )
    ]
    for load in loads:
        load.start()

    def to_patches(src, dst, k):
        def step(i, carry):
            q = peer(i)
            pltpu.make_async_remote_copy(
                src_ref=src.at[q], dst_ref=dst.at[p], send_sem=ssem.at[k], recv_sem=rsem.at[k],
                device_id={"patch": q}, device_id_type=MESH,
            ).start()
            return carry

        lax.fori_loop(1, np_, step, 0)
        dst[p] = src[p]

    def to_bands(src, dst, k, same):
        def step(i, carry):
            q = level(i)
            pltpu.make_async_remote_copy(
                src_ref=src if same else src.at[q], dst_ref=dst.at[b],
                send_sem=ssem.at[k], recv_sem=rsem.at[k],
                device_id={"band": q}, device_id_type=MESH,
            ).start()
            return carry

        lax.fori_loop(1, nb, step, 0)
        dst[b] = src[...] if same else src[b]

    def settle(dst, sems, k):
        view = dst.at[pl.ds(0, dst.shape[0] - 1)]
        pltpu.make_async_copy(view, view, sems.at[k]).wait()

    target = tgt[...]
    named = mark(iota((np_, edges), 0) == target)
    before = mark(iota((edges, edges), 0) < iota((edges, edges), 1))
    rank = mm(named, before)
    slot = jnp.sum(rank * named.astype(F32), axis=0, keepdims=True).astype(I32)
    chosen = mark(iota((slots, edges), 0) == target * CAP + slot)
    lanes = iota((128, edges), 0)
    mine = (lanes % CAP == slot) & (lanes // CAP == p % 16)
    node = nod[...] + 1
    high = jnp.where(mine, (node >> 6).astype(F32), 0.0).astype(BF16)
    low = jnp.where(mine, (node & 63).astype(F32), 0.0).astype(BF16)
    addr_out[:, 0, :] = 64.0 * mm_rows(named, high) + mm_rows(named, low)
    from_grid = mm_rows(chosen, mark(iota((grid_rows, edges), 0) == snd[...])).astype(BF16)
    geo_rows = mm_rows(chosen, geo[...]).astype(BF16)

    loads[0].wait()
    loads[1].wait()
    hidden = silu(mm(gf[...], gi[...])).astype(BF16)
    loads[2].wait()
    latent = norm_rows(mm(hidden, go[...])).astype(BF16)
    loads[3].wait()
    sender_proj = mm(latent, ee[0]).astype(BF16)
    terms = mm(from_grid, sender_proj) + mm(geo_rows, gw[...])
    outbox[...] = terms.reshape(np_, CAP, width).astype(BF16)

    pl.semaphore_wait(barrier, np_ + nb - 2)
    to_patches(addr_out, addr_in, 0)
    to_patches(outbox, inbox, 1)

    loads[4].wait()
    recv_proj[...] = mm(mn[...], ee[1]).astype(BF16)
    loads[5].wait()
    loads[6].wait()
    edge_proj[...] = mm(me[...], pe[0])
    loads[7].wait()
    loads[8].wait()
    row = iota((padded, count), 0)
    own_pick = mark((iota((padded, count), 1) == b * share + row) & (row < share))
    own = mm(own_pick, mn[...]).astype(BF16)
    own_proj = mm(own, en[0])
    row, col = iota((padded, block), 0), iota((padded, block), 1)
    to_left = mark((row == col) & (row < share))
    to_right = mark(col == row + share)
    row, col = iota((block, padded), 0), iota((block, padded), 1)
    from_left = mark((row == col) & (row < share))
    from_right = mark(row == col + share)
    where_row = iota((wide, 1), 0).astype(F32)
    where_band = jnp.floor((where_row + 0.5) * (1.0 / block))
    within = where_row - block * where_band
    wide_node = where_band * share + jnp.where(within < share, within, within - share)
    left_rows = jnp.broadcast_to(within, (wide, half)) < share

    def in_halves(rows):
        picked = jnp.where(left_rows, rows[:, :half], rows[:, half:])
        return picked.reshape(nb, block, half).astype(BF16)

    def update(rows, rows_proj, arrived, weights):
        agg = jnp.sum(arrived[...].astype(F32), axis=0).astype(BF16)
        agg_left = mm(to_left, agg).astype(BF16)
        agg_right = mm(to_right, agg).astype(BF16)
        preact = rows_proj + mm(agg_left, weights[1, :half]) + mm(agg_right, weights[1, half:])
        return (rows.astype(F32) + tail(preact, weights[2])).astype(BF16)

    def packed(rows):
        return (mm(from_left, rows[:, :half]) + mm(from_right, rows[:, half:])).astype(BF16)

    def natural(arrived, out):
        flat = arrived[...].astype(F32).reshape(wide, half).astype(BF16)
        row = iota((count, wide), 0).astype(F32)
        place = row + share * jnp.floor((row + 0.5) * (1.0 / share))
        col = iota((count, wide), 1).astype(F32)
        out[:, :half] = mm(mark(col == place), flat).astype(BF16)
        out[:, half:] = mm(mark(col == place + share), flat).astype(BF16)

    settle(addr_in, rsem, 0)
    per = min(16, np_)
    placed = jnp.sum(addr_in[:, 0, :].reshape(np_ // per, per, 128), axis=1)
    span = per * CAP
    pieces = [placed[k : k + 1, :span] for k in range(np_ // per)]
    node_rows = iota((count, span), 0).astype(F32) + 1.0
    landing = jnp.concatenate([mark(node_rows == v) for v in pieces], axis=1)
    wide_landing = jnp.concatenate(
        [mark(jnp.broadcast_to(wide_node + 1.0, (wide, span)) == v) for v in pieces], axis=1
    )
    gathered = mm_cols(landing, recv_proj[...])

    settle(inbox, rsem, 1)
    preact = inbox[...].astype(F32).reshape(slots, width) + gathered
    message = tail(preact, ee[2]).astype(BF16)
    rs_out[...] = in_halves(mm(wide_landing, message))
    to_bands(rs_out, rs_in, 2, False)
    settle(rs_in, rsem, 2)
    first = update(own, own_proj, rs_in, en)
    ag_out[...] = packed(first)
    to_bands(ag_out, ag_in, 3, True)
    first_proj = mm(first, pn[0])

    spread_to = iota((np_ * 4, slots), 1)
    spread_from = iota((np_ * 4, slots), 0)
    spread = mark(spread_from == (spread_to >> 3) * 4 + (spread_to & 3))
    rows = jnp.broadcast_to(halo[...], (8, np_ * 4))
    wanted = 64.0 * mm((rows >> 6).astype(F32).astype(BF16), spread) + mm(
        (rows & 63).astype(F32).astype(BF16), spread
    )
    halo_pick = mark(iota((count, slots), 0).astype(F32) == wanted[0:1, :])
    left_slots = (iota((slots, half), 0) & 7) < 4
    local_pick = mark(iota((count, medges), 0) == msd[...])
    recv_pick = mark(iota((count, medges), 0) == mrc[...])
    ghost = msd[...] - count
    ghost_row = jnp.where(ghost < 0, -1024, (ghost >> 2) * 8 + (ghost & 3))
    ghost_left = mark(iota((slots, medges), 0) == ghost_row)
    ghost_right = mark(iota((slots, medges), 0) == ghost_row + 4)
    wide_recv = mark(
        jnp.broadcast_to(wide_node, (wide, medges)) == mrc[...].astype(F32)
    )

    settle(ag_in, rsem, 3)
    natural(ag_in, one_ref)
    sent = mm(one_ref[...], pe[1]).astype(BF16)
    going = mm_cols(halo_pick, sent)
    going = jnp.where(left_slots, going[:, :half], going[:, half:])
    halo_out[...] = going.reshape(np_, CAP, half).astype(BF16)
    to_patches(halo_out, halo_in, 4)
    recv_two = mm(one_ref[...], pe[2]).astype(BF16)
    edge_proj[...] += mm_cols(local_pick, sent) + mm_cols(recv_pick, recv_two)

    settle(halo_in, rsem, 4)
    ghosts = halo_in[...].astype(F32).reshape(slots, half).astype(BF16)
    edge_proj[:, :half] += mm_cols(ghost_left, ghosts)
    edge_proj[:, half:] += mm_cols(ghost_right, ghosts)
    edge_new = (me[...].astype(F32) + tail(edge_proj[...], pe[3])).astype(BF16)
    rs2_out[...] = in_halves(mm(wide_recv, edge_new))
    to_bands(rs2_out, rs2_in, 5, False)
    edge_ref[...] = edge_new
    settle(rs2_in, rsem, 5)
    second = update(first, first_proj, rs2_in, pn)
    ag2_out[...] = packed(second)
    to_bands(ag2_out, ag2_in, 6, True)
    settle(ag2_in, rsem, 6)
    natural(ag2_in, two_ref)

    settle(addr_in, ssem, 0)
    settle(inbox, ssem, 1)
    settle(rs_in, ssem, 2)
    settle(ag_in, ssem, 3)
    settle(halo_in, ssem, 4)
    settle(rs2_in, ssem, 5)
    settle(ag2_in, ssem, 6)


def per_device(
    nb, np_, ny,
    grid_feat, enc_sender, enc_patch, enc_node, enc_geo, mesh_nodes, mesh_edge, mesh_send,
    mesh_recv, halo_rows, grid_in, grid_out, geo_weight, enc_edge_w, enc_node_w, proc_edge_w,
    proc_node_w,
):
    edges = enc_sender.shape[0]
    count, width = mesh_nodes.shape
    medges = mesh_edge.shape[0]
    half = width // 2
    block = 2 * count // nb
    slots = np_ * CAP
    whole = pl.BlockSpec(memory_space=pltpu.VMEM)
    away = pl.BlockSpec(memory_space=pl.ANY)

    def like(v):
        return pltpu.VMEM(v.shape, v.dtype)

    return pl.pallas_call(
        functools.partial(kernel, nb, np_, ny),
        out_shape=(
            jax.ShapeDtypeStruct((count, width), BF16),
            jax.ShapeDtypeStruct((medges, width), BF16),
        ),
        in_specs=[away] * 3 + [whole] + [away] * 6 + [whole] * 7,
        out_specs=(whole, whole),
        scratch_shapes=[
            like(grid_feat), like(grid_in), like(grid_out), like(enc_edge_w), like(enc_node_w),
            like(proc_edge_w), like(proc_node_w), like(mesh_nodes), like(mesh_edge),
            pltpu.SemaphoreType.DMA((9,)),
            pltpu.VMEM((np_, 1, 128), F32), pltpu.VMEM((np_, 1, 128), F32),
            pltpu.VMEM((np_, CAP, width), BF16), pltpu.VMEM((np_, CAP, width), BF16),
            pltpu.VMEM((nb, block, half), BF16), pltpu.VMEM((nb, block, half), BF16),
            pltpu.VMEM((block, half), BF16), pltpu.VMEM((nb, block, half), BF16),
            pltpu.VMEM((np_, CAP, half), BF16), pltpu.VMEM((np_, CAP, half), BF16),
            pltpu.VMEM((nb, block, half), BF16), pltpu.VMEM((nb, block, half), BF16),
            pltpu.VMEM((block, half), BF16), pltpu.VMEM((nb, block, half), BF16),
            pltpu.VMEM((count, width), BF16), pltpu.VMEM((medges, width), F32),
            pltpu.VMEM((count, width), BF16),
            pltpu.SemaphoreType.DMA((7,)), pltpu.SemaphoreType.DMA((7,)),
        ],
        compiler_params=pltpu.CompilerParams(collective_id=0, has_side_effects=True),
    )(
        grid_feat, grid_in, grid_out, geo_weight, enc_edge_w, enc_node_w, proc_edge_w,
        proc_node_w, mesh_nodes, mesh_edge,
        enc_patch.reshape(1, edges), enc_sender.reshape(1, edges), enc_node.reshape(1, edges),
        enc_geo, mesh_send.reshape(1, medges), mesh_recv.reshape(1, medges), halo_rows,
    )


def solution(mesh):
    both = ("band", "patch")
    nb, np_ = mesh.shape["band"], mesh.shape["patch"]
    ny = 8 if np_ == 64 else np_ // 4
    placed = (
        P(both, None), P(both), P(both, None), P(both), P(None, both), P("patch", None),
        P(both, None), P(both), P(both), P("patch", None),
    ) + (P(),) * 7
    return jax.shard_map(
        functools.partial(per_device, nb, np_, ny),
        mesh=mesh,
        in_specs=placed,
        out_specs=(P("patch", None), P(both, None)),
        check_vma=False,
    )
```

```python
import functools

import jax
import jax.numpy as jnp
from jax import lax
from jax.experimental import pallas as pl
from jax.experimental.pallas import tpu as pltpu
from jax.sharding import PartitionSpec as P

F32 = jnp.float32
BF16 = jnp.bfloat16
I32 = jnp.int32
MESH = pl.DeviceIdType.MESH
CAP = 8


def mark(condition):
    return jnp.where(condition, 1.0, 0.0).astype(BF16)


def iota(shape, dim):
    return lax.broadcasted_iota(I32, shape, dim)


def mm(a, b):
    return jnp.dot(a, b, preferred_element_type=F32)


def mm_rows(a, b):
    return lax.dot_general(a, b, (((1,), (1,)), ((), ())), preferred_element_type=F32)


def mm_cols(a, b):
    return lax.dot_general(a, b, (((0,), (0,)), ((), ())), preferred_element_type=F32)


def norm_rows(v):
    centred = v - jnp.mean(v, axis=-1, keepdims=True)
    spread = jnp.mean(centred * centred, axis=-1, keepdims=True)
    return centred * lax.rsqrt(spread + 1e-05)


def silu(v):
    return v * jax.nn.sigmoid(v)


def tail(preact, weight):
    return norm_rows(mm(silu(preact).astype(BF16), weight))


def kernel(
    nb, np_, ny,
    gf_h, gi_h, go_h, gw, ee_h, en_h, pe_h, pn_h, mn_h, me_h,
    tgt, snd, nod, geo, msd, mrc, halo,
    two_ref, edge_ref,
    gf, gi, go, ee, en, pe, pn, mn, me, wsem,
    addr_out, addr_in, outbox, inbox, rs_out, rs_in, ag_out, ag_in,
    halo_out, halo_in, rs2_out, rs2_in, ag2_out, ag2_in,
    via_in, via_out, via2_in, via2_out, left_pick, right_pick,
    recv_proj, edge_proj, one_ref, placed, total, ssem, rsem,
):
    b = lax.axis_index("band")
    p = lax.axis_index("patch")
    edges = tgt.shape[1]
    count, width = mn.shape
    half = width // 2
    share = count // nb
    block = 2 * share
    slots = np_ * CAP
    grid_rows = gf.shape[1]
    medges = me.shape[0]
    padded = -(-share // 16) * 16
    cut = -(-share // 8) * 8
    wide = 2 * count

    per = 2 * ny
    nx = np_ // per
    x0, y0, c0 = p // per, (p // 2) % ny, p % 2
    steps = [(ny // 2 + (k + 1) // 2 * (1 if k % 2 else -1)) % ny for k in range(ny)]
    spots = [
        ((dy, c), (y0 + dy) % ny * 2 + (c0 + c) % 2) for dy in steps for c in range(2)
    ]

    def each_peer(visit):
        for where, spot in spots:
            if where != (0, 0):
                visit(x0 * per + spot, 0)

        def column(dx, carry):
            first = (x0 + dx) % nx * per
            for _, spot in spots:
                visit(first + spot, dx)
            return carry

        lax.fori_loop(1, nx, column, 0)

    loads = [
        pltpu.make_async_copy(src, dst, wsem.at[k])
        for k, (src, dst) in enumerate(
            [(gf_h, gf), (gi_h, gi), (go_h, go), (ee_h, ee), (mn_h, mn), (me_h, me),
             (pe_h, pe), (en_h, en), (pn_h, pn)]
        )
    ]
    for load in loads:
        load.start()

    barrier = pltpu.get_barrier_semaphore()

    def greet(axis, q):
        pl.semaphore_signal(barrier, inc=1, device_id={axis: q}, device_id_type=MESH)

    each_peer(lambda q, dx: greet("patch", q))
    for k in range(1, nb):
        greet("band", (b + k) % nb)

    def to_patches(src, dst, send, recv, apart):
        def visit(q, dx):
            pltpu.make_async_remote_copy(
                src_ref=src.at[q], dst_ref=dst.at[p], send_sem=ssem.at[send],
                recv_sem=rsem.at[recv + dx if apart else recv],
                device_id={"patch": q}, device_id_type=MESH,
            ).start()

        each_peer(visit)
        dst[p] = src[p]

    sides = ((0, 1, pl.ds(0, cut)), (1, -1, pl.ds(cut, block - cut)))

    def to_band(src, dst, send, recv, q):
        pltpu.make_async_remote_copy(
            src_ref=src, dst_ref=dst, send_sem=ssem.at[send], recv_sem=rsem.at[recv],
            device_id={"band": q}, device_id_type=MESH,
        ).start()

    def wait_for(view, sem):
        pltpu.make_async_copy(view, view, sem).wait()

    def reduce_bands(src, via, sums, dst, send, recv, last):
        for k in (4, 3, 2, 1):
            for side, sign, rows in sides:
                q = (b + nb - sign * k) % nb
                o = (b + nb - sign * (k + 4)) % nb
                if k == 4:
                    to_band(src.at[o, rows], via.at[6, rows], send, last + side, q)
                else:
                    to_band(src.at[o], via.at[side * 3 + k - 1], send, recv + side, q)
        for k in (3, 2, 1):
            for side, sign, rows in sides:
                q = (b + nb - sign * k) % nb
                to_band(src.at[q], dst.at[side * 3 + k - 1], send, recv + 2, q)
        for side, sign, rows in sides:
            q = (b + nb - sign * 4) % nb
            wait_for(via.at[pl.ds(0, 3)], rsem.at[recv + side])
            wait_for(via.at[6, rows], rsem.at[last + side])
            value = src[q].astype(F32)
            for k in range(3):
                value = value + via[side * 3 + k].astype(F32)
            sums[side] = value.astype(BF16)
            part = slice(rows.start, rows.start + rows.size)
            sums[side, part] = (value[part] + via[6, part].astype(F32)).astype(BF16)
            to_band(sums.at[side], dst.at[6 + side], send, recv + 2, q)

    def reduced(src, dst, recv):
        wait_for(dst.at[pl.ds(0, 8)], rsem.at[recv + 2])
        return src[b].astype(F32) + jnp.sum(dst[...].astype(F32), axis=0)

    def gather_bands(src, dst, send, recv):
        for k in (4, 3, 2, 1):
            for side, sign, rows in sides:
                sem = recv + side if k == 4 else recv + 2
                to_band(src, dst.at[b], send, sem, (b + nb + sign * k) % nb)
        dst[b] = src[...]

    def relay_bands(dst, send, recv):
        for side, sign, rows in sides:
            o = (b + nb - sign * 4) % nb
            wait_for(dst.at[0], rsem.at[recv + side])
            to_band(dst.at[o, rows], dst.at[o, rows], send, recv + 2, (b + nb + sign * 4) % nb)
            for k in (3, 2, 1):
                to_band(dst.at[o], dst.at[o], send, recv + 2, (b + nb + sign * k) % nb)

    def settle(dst, sems, k):
        view = dst.at[pl.ds(0, dst.shape[0] - 1)]
        pltpu.make_async_copy(view, view, sems.at[k]).wait()

    target = tgt[...]
    named = mark(iota((np_, edges), 0) == target)
    before = mark(iota((edges, edges), 0) < iota((edges, edges), 1))
    rank = mm(named, before)
    slot = jnp.sum(rank * named.astype(F32), axis=0, keepdims=True).astype(I32)
    chosen = mark(iota((slots, edges), 0) == target * CAP + slot)
    lanes = iota((128, edges), 0)
    mine = (lanes % CAP == slot) & (lanes // CAP == p % per)
    node = nod[...].reshape(1, edges) + 1
    high = jnp.where(mine, (node >> 6).astype(F32), 0.0).astype(BF16)
    low = jnp.where(mine, (node & 63).astype(F32), 0.0).astype(BF16)
    addr_out[:, 0, :] = 64.0 * mm_rows(named, high) + mm_rows(named, low)
    from_grid = mm_rows(chosen, mark(iota((grid_rows, edges), 0) == snd[...].reshape(1, edges))).astype(BF16)
    geo_rows = mm_rows(chosen, geo[...]).astype(BF16)

    loads[0].wait()
    loads[1].wait()
    hidden = silu(mm_cols(gf[...], gi[...])).astype(BF16)
    loads[2].wait()
    latent = norm_rows(mm(hidden, go[...])).astype(BF16)
    loads[3].wait()
    sender_proj = mm(latent, ee[0]).astype(BF16)
    terms = mm(from_grid, sender_proj) + mm(geo_rows, gw[...])
    outbox[...] = terms.reshape(np_, CAP, width).astype(BF16)

    pl.semaphore_wait(barrier, np_ + nb - 2)
    to_patches(addr_out, addr_in, 0, 0, False)
    to_patches(outbox, inbox, 1, 19, True)

    loads[4].wait()
    recv_proj[...] = mm(mn[...], ee[1]).astype(BF16)
    loads[5].wait()
    loads[6].wait()
    edge_proj[...] = mm(me[...], pe[0])
    loads[7].wait()
    loads[8].wait()
    row = iota((padded, count), 0)
    own_pick = mark((iota((padded, count), 1) == b * share + row) & (row < share))
    own = mm(own_pick, mn[...]).astype(BF16)
    own_proj = mm(own, en[0])
    row, col = iota((padded, block), 0), iota((padded, block), 1)
    to_left = mark((row == col) & (row < share))
    to_right = mark(col == row + share)
    row, col = iota((block, padded), 0), iota((block, padded), 1)
    from_left = mark((row == col) & (row < share))
    from_right = mark(row == col + share)
    where_row = iota((wide, 1), 0).astype(F32)
    where_band = jnp.floor((where_row + 0.5) * (1.0 / block))
    within = where_row - block * where_band
    wide_node = where_band * share + jnp.where(within < share, within, within - share)
    left_rows = jnp.broadcast_to(within, (wide, half)) < share

    def in_halves(rows):
        picked = jnp.where(left_rows, rows[:, :half], rows[:, half:])
        return picked.reshape(nb, block, half).astype(BF16)

    def update(rows, rows_proj, arrived, weights):
        agg = arrived.astype(BF16)
        agg_left = mm(to_left, agg).astype(BF16)
        agg_right = mm(to_right, agg).astype(BF16)
        preact = rows_proj + mm(agg_left, weights[1, :half]) + mm(agg_right, weights[1, half:])
        return (rows.astype(F32) + tail(preact, weights[2])).astype(BF16)

    def packed(rows):
        return (mm(from_left, rows[:, :half]) + mm(from_right, rows[:, half:])).astype(BF16)

    row = iota((count, wide), 0).astype(F32)
    place = row + share * jnp.floor((row + 0.5) * (1.0 / share))
    col = iota((count, wide), 1).astype(F32)
    left_pick[...] = mark(col == place)
    right_pick[...] = mark(col == place + share)

    def natural(arrived, out):
        flat = arrived[...].astype(F32).reshape(wide, half).astype(BF16)
        out[:, :half] = mm(left_pick[...], flat).astype(BF16)
        out[:, half:] = mm(right_pick[...], flat).astype(BF16)

    settle(addr_in, rsem, 0)
    span = per * CAP
    placed[:, 0, :] = jnp.sum(addr_in[:, 0, :].reshape(nx, per, 128), axis=1)
    node_rows = iota((count, span), 0).astype(F32) + 1.0
    wide_rows = jnp.broadcast_to(wide_node + 1.0, (wide, span))
    for dx in range(nx):
        x = (x0 + nx - dx) % nx
        names = placed[x][:, :span]
        gathered = mm_cols(mark(node_rows == names), recv_proj[...])
        wide_landing = mark(wide_rows == names)
        wait_for(inbox.at[pl.ds(0, per - 1 if dx == 0 else per)], rsem.at[19 + dx])
        arrived = inbox[pl.ds(x * per, per)].astype(F32).reshape(span, width)
        message = tail(arrived + gathered, ee[2]).astype(BF16)
        landed = mm(wide_landing, message)
        if dx == 0:
            total[...] = landed
        elif dx < nx - 1:
            total[...] += landed
        else:
            rs_out[...] = in_halves(total[...] + landed)
    reduce_bands(rs_out, via_in, via_out, rs_in, 2, 7, 19 + nx)
    first = update(own, own_proj, reduced(rs_out, rs_in, 7), en)
    ag_out[...] = packed(first)
    gather_bands(ag_out, ag_in, 3, 10)
    relay_bands(ag_in, 3, 10)
    first_proj = mm(first, pn[0])

    spread_to = iota((np_ * 4, slots), 1)
    spread_from = iota((np_ * 4, slots), 0)
    spread = mark(spread_from == (spread_to >> 3) * 4 + (spread_to & 3))
    rows = jnp.broadcast_to(halo[...], (8, np_ * 4))
    wanted = 64.0 * mm((rows >> 6).astype(F32).astype(BF16), spread) + mm(
        (rows & 63).astype(F32).astype(BF16), spread
    )
    halo_pick = mark(iota((count, slots), 0).astype(F32) == wanted[0:1, :])
    left_slots = (iota((slots, half), 0) & 7) < 4
    local_pick = mark(iota((count, medges), 0) == msd[...])
    recv_pick = mark(iota((count, medges), 0) == mrc[...])
    ghost = msd[...] - count
    ghost_row = jnp.where(ghost < 0, -1024, (ghost >> 2) * 8 + (ghost & 3))
    ghost_left = mark(iota((slots, medges), 0) == ghost_row)
    ghost_right = mark(iota((slots, medges), 0) == ghost_row + 4)
    wide_recv = mark(
        jnp.broadcast_to(wide_node, (wide, medges)) == mrc[...].astype(F32)
    )

    wait_for(ag_in.at[pl.ds(0, 13)], rsem.at[12])
    natural(ag_in, one_ref)
    sent = mm(one_ref[...], pe[1]).astype(BF16)
    going = mm_cols(halo_pick, sent)
    going = jnp.where(left_slots, going[:, :half], going[:, half:])
    halo_out[...] = going.reshape(np_, CAP, half).astype(BF16)
    to_patches(halo_out, halo_in, 4, 4, False)
    recv_two = mm(one_ref[...], pe[2]).astype(BF16)
    edge_proj[...] += mm_cols(local_pick, sent) + mm_cols(recv_pick, recv_two)

    settle(halo_in, rsem, 4)
    ghosts = halo_in[...].astype(F32).reshape(slots, half).astype(BF16)
    edge_proj[:, :half] += mm_cols(ghost_left, ghosts)
    edge_proj[:, half:] += mm_cols(ghost_right, ghosts)
    edge_new = (me[...].astype(F32) + tail(edge_proj[...], pe[3])).astype(BF16)
    rs2_out[...] = in_halves(mm(wide_recv, edge_new))
    reduce_bands(rs2_out, via2_in, via2_out, rs2_in, 5, 13, 21 + nx)
    edge_ref[...] = edge_new
    second = update(first, first_proj, reduced(rs2_out, rs2_in, 13), pn)
    ag2_out[...] = packed(second)
    gather_bands(ag2_out, ag2_in, 6, 16)
    relay_bands(ag2_in, 6, 16)
    wait_for(ag2_in.at[pl.ds(0, 13)], rsem.at[18])
    natural(ag2_in, two_ref)

    settle(addr_in, ssem, 0)
    settle(inbox, ssem, 1)
    settle(rs_out, ssem, 2)
    settle(ag_in, ssem, 3)
    settle(halo_in, ssem, 4)
    settle(rs2_out, ssem, 5)
    settle(ag2_in, ssem, 6)


def per_device(
    nb, np_, ny,
    grid_feat, enc_sender, enc_patch, enc_node, enc_geo, mesh_nodes, mesh_edge, mesh_send,
    mesh_recv, halo_rows, grid_in, grid_out, geo_weight, enc_edge_w, enc_node_w, proc_edge_w,
    proc_node_w,
):
    edges = enc_sender.shape[0]
    count, width = mesh_nodes.shape
    medges = mesh_edge.shape[0]
    half = width // 2
    block = 2 * count // nb
    slots = np_ * CAP
    whole = pl.BlockSpec(memory_space=pltpu.VMEM)
    away = pl.BlockSpec(memory_space=pl.ANY)

    def like(v):
        return pltpu.VMEM(v.shape, v.dtype)

    return pl.pallas_call(
        functools.partial(kernel, nb, np_, ny),
        out_shape=(
            pltpu.VMEM((count, width), BF16),
            pltpu.VMEM((medges, width), BF16),
        ),
        in_specs=[away] * 3 + [whole] + [away] * 6 + [whole] * 7,
        out_specs=(whole, whole),
        scratch_shapes=[
            pltpu.VMEM(grid_feat.shape[::-1], BF16), like(grid_in), like(grid_out), like(enc_edge_w), like(enc_node_w),
            like(proc_edge_w), like(proc_node_w), like(mesh_nodes), like(mesh_edge),
            pltpu.SemaphoreType.DMA((9,)),
            pltpu.VMEM((np_, 1, 128), F32), pltpu.VMEM((np_, 1, 128), F32),
            pltpu.VMEM((np_, CAP, width), BF16), pltpu.VMEM((np_, CAP, width), BF16),
            pltpu.VMEM((nb, block, half), BF16), pltpu.VMEM((8, block, half), BF16),
            pltpu.VMEM((block, half), BF16), pltpu.VMEM((nb, block, half), BF16),
            pltpu.VMEM((np_, CAP, half), BF16), pltpu.VMEM((np_, CAP, half), BF16),
            pltpu.VMEM((nb, block, half), BF16), pltpu.VMEM((8, block, half), BF16),
            pltpu.VMEM((block, half), BF16), pltpu.VMEM((nb, block, half), BF16),
            pltpu.VMEM((7, block, half), BF16), pltpu.VMEM((2, block, half), BF16),
            pltpu.VMEM((7, block, half), BF16), pltpu.VMEM((2, block, half), BF16),
            pltpu.VMEM((count, 2 * count), BF16), pltpu.VMEM((count, 2 * count), BF16),
            pltpu.VMEM((count, width), BF16), pltpu.VMEM((medges, width), F32),
            pltpu.VMEM((count, width), BF16),
            pltpu.VMEM((np_ // (2 * ny), 1, 128), F32), pltpu.VMEM((2 * count, width), F32),
            pltpu.SemaphoreType.DMA((7,)), pltpu.SemaphoreType.DMA((23 + np_ // (2 * ny),)),
        ],
        compiler_params=pltpu.CompilerParams(collective_id=0, has_side_effects=True),
    )(
        grid_feat.T, grid_in, grid_out, geo_weight, enc_edge_w, enc_node_w, proc_edge_w,
        proc_node_w, mesh_nodes, mesh_edge,
        enc_patch.reshape(1, edges), enc_sender, enc_node,
        enc_geo, mesh_send.reshape(1, medges), mesh_recv.reshape(1, medges), halo_rows,
    )


def solution(mesh):
    both = ("band", "patch")
    nb, np_ = mesh.shape["band"], mesh.shape["patch"]
    ny = 8 if np_ == 64 else np_ // 4
    placed = (
        P(both, None), P(both), P(both, None), P(both), P(None, both), P("patch", None),
        P(both, None), P(both), P(both), P("patch", None),
    ) + (P(),) * 7
    return jax.shard_map(
        functools.partial(per_device, nb, np_, ny),
        mesh=mesh,
        in_specs=placed,
        out_specs=(P("patch", None), P(both, None)),
        check_vma=False,
    )
```

```python
import functools

import jax
import jax.numpy as jnp
from jax import lax
from jax.experimental import pallas as pl
from jax.experimental.pallas import tpu as pltpu
from jax.sharding import PartitionSpec as P

F32 = jnp.float32
BF16 = jnp.bfloat16
I32 = jnp.int32
MESH = pl.DeviceIdType.MESH
CAP = 8


def mark(condition):
    return jnp.where(condition, 1.0, 0.0).astype(BF16)


def iota(shape, dim):
    return lax.broadcasted_iota(I32, shape, dim)


def mm(a, b):
    return jnp.dot(a, b, preferred_element_type=F32)


def mm_rows(a, b):
    return lax.dot_general(a, b, (((1,), (1,)), ((), ())), preferred_element_type=F32)


def mm_cols(a, b):
    return lax.dot_general(a, b, (((0,), (0,)), ((), ())), preferred_element_type=F32)


def norm_rows(v):
    centred = v - jnp.mean(v, axis=-1, keepdims=True)
    spread = jnp.mean(centred * centred, axis=-1, keepdims=True)
    return centred * lax.rsqrt(spread + 1e-05)


def silu(v):
    return v * jax.nn.sigmoid(v)


def tail(preact, weight):
    return norm_rows(mm(silu(preact).astype(BF16), weight))


def kernel(
    nb, np_, ny,
    gf_h, gi_h, go_h, gw, ee_h, en_h, pe_h, pn_h, mn_h, me_h,
    tgt, snd, nod, geo, msd, mrc, halo,
    two_ref, edge_ref,
    gf, gi, go, ee, en, pe, pn, mn, me, wsem,
    addr_out, addr_in, outbox, inbox, rs_out, rs_in, ag_out, ag_in,
    halo_out, halo_in, rs2_out, rs2_in, ag2_out, ag2_in,
    via_in, via_out, via2_in, via2_out, left_pick, right_pick,
    recv_proj, edge_proj, one_ref, placed, total, grid_pick, geo_pick, ssem, rsem,
):
    b = lax.axis_index("band")
    p = lax.axis_index("patch")
    edges = tgt.shape[1]
    count, width = mn.shape
    half = width // 2
    share = count // nb
    block = 2 * share
    slots = np_ * CAP
    grid_rows = gf.shape[1]
    medges = me.shape[0]
    padded = -(-share // 16) * 16
    cut = -(-share // 8) * 8
    wide = 2 * count

    per = 2 * ny
    nx = np_ // per
    x0, y0, c0 = p // per, (p // 2) % ny, p % 2
    steps = [(ny // 2 + (k + 1) // 2 * (1 if k % 2 else -1)) % ny for k in range(ny)]
    spots = [
        ((dy, c), (y0 + dy) % ny * 2 + (c0 + c) % 2) for dy in steps for c in range(2)
    ]

    def each_peer(visit):
        for where, spot in spots:
            if where != (0, 0):
                visit(x0 * per + spot, 0)

        def column(dx, carry):
            first = (x0 + dx) % nx * per
            for _, spot in spots:
                visit(first + spot, dx)
            return carry

        lax.fori_loop(1, nx, column, 0)

    loads = [
        pltpu.make_async_copy(src, dst, wsem.at[k])
        for k, (src, dst) in enumerate(
            [(gf_h, gf), (gi_h, gi), (go_h, go), (ee_h, ee), (mn_h, mn), (me_h, me),
             (pe_h, pe), (en_h, en), (pn_h, pn)]
        )
    ]
    for load in loads:
        load.start()

    barrier = pltpu.get_barrier_semaphore()

    def greet(axis, q):
        pl.semaphore_signal(barrier, inc=1, device_id={axis: q}, device_id_type=MESH)

    for k in range(nb // 2, 0, -1):
        greet("band", (b + k) % nb)
        if 2 * k != nb:
            greet("band", (b + nb - k) % nb)
    each_peer(lambda q, dx: greet("patch", q))

    def to_patches(src, dst, send, recv):
        def visit(q, dx):
            pltpu.make_async_remote_copy(
                src_ref=src.at[q], dst_ref=dst.at[p], send_sem=ssem.at[send],
                recv_sem=rsem.at[recv],
                device_id={"patch": q}, device_id_type=MESH,
            ).start()

        each_peer(visit)
        dst[p] = src[p]

    def to_column(src, dst, send, recv, dx):
        first = (x0 + dx) % nx * per
        for where, spot in spots:
            if dx or where != (0, 0):
                q = first + spot
                pltpu.make_async_remote_copy(
                    src_ref=src.at[q], dst_ref=dst.at[p], send_sem=ssem.at[send],
                    recv_sem=rsem.at[recv + dx], device_id={"patch": q}, device_id_type=MESH,
                ).start()

    sides = ((0, 1, pl.ds(0, cut)), (1, -1, pl.ds(cut, block - cut)))

    def to_band(src, dst, send, recv, q):
        pltpu.make_async_remote_copy(
            src_ref=src, dst_ref=dst, send_sem=ssem.at[send], recv_sem=rsem.at[recv],
            device_id={"band": q}, device_id_type=MESH,
        ).start()

    def wait_for(view, sem):
        pltpu.make_async_copy(view, view, sem).wait()

    def reduce_bands(src, via, sums, dst, send, recv, last):
        for k in (4, 3, 2, 1):
            for side, sign, rows in sides:
                q = (b + nb - sign * k) % nb
                o = (b + nb - sign * (k + 4)) % nb
                if k == 4:
                    to_band(src.at[o, rows], via.at[6, rows], send, last + side, q)
                else:
                    to_band(src.at[o], via.at[side * 3 + k - 1], send, recv + side, q)
        for k in (3, 2, 1):
            for side, sign, rows in sides:
                q = (b + nb - sign * k) % nb
                to_band(src.at[q], dst.at[side * 3 + k - 1], send, recv + 2, q)
        for side, sign, rows in sides:
            q = (b + nb - sign * 4) % nb
            wait_for(via.at[pl.ds(0, 3)], rsem.at[recv + side])
            wait_for(via.at[6, rows], rsem.at[last + side])
            value = src[q].astype(F32)
            for k in range(3):
                value = value + via[side * 3 + k].astype(F32)
            sums[side] = value.astype(BF16)
            part = slice(rows.start, rows.start + rows.size)
            sums[side, part] = (value[part] + via[6, part].astype(F32)).astype(BF16)
            to_band(sums.at[side], dst.at[6 + side], send, recv + 2, q)

    def reduced(src, dst, recv):
        wait_for(dst.at[pl.ds(0, 8)], rsem.at[recv + 2])
        return src[b].astype(F32) + jnp.sum(dst[...].astype(F32), axis=0)

    def gather_bands(src, dst, send, recv):
        for k in (4, 3, 2, 1):
            for side, sign, rows in sides:
                sem = recv + side if k == 4 else recv + 2
                to_band(src, dst.at[b], send, sem, (b + nb + sign * k) % nb)
        dst[b] = src[...]

    def relay_bands(dst, send, recv):
        for side, sign, rows in sides:
            o = (b + nb - sign * 4) % nb
            wait_for(dst.at[0], rsem.at[recv + side])
            to_band(dst.at[o, rows], dst.at[o, rows], send, recv + 2, (b + nb + sign * 4) % nb)
            for k in (3, 2, 1):
                to_band(dst.at[o], dst.at[o], send, recv + 2, (b + nb + sign * k) % nb)

    def settle(dst, sems, k):
        view = dst.at[pl.ds(0, dst.shape[0] - 1)]
        pltpu.make_async_copy(view, view, sems.at[k]).wait()

    target = tgt[...]
    named = mark(iota((np_, edges), 0) == target)
    before = mark(iota((edges, edges), 0) < iota((edges, edges), 1))
    rank = mm(named, before)
    slot = jnp.sum(rank * named.astype(F32), axis=0, keepdims=True).astype(I32)
    chosen = mark(iota((slots, edges), 0) == target * CAP + slot)
    lanes = iota((128, edges), 0)
    mine = (lanes % CAP == slot) & (lanes // CAP == p % per)
    node = nod[...].reshape(1, edges) + 1
    high = jnp.where(mine, (node >> 6).astype(F32), 0.0).astype(BF16)
    low = jnp.where(mine, (node & 63).astype(F32), 0.0).astype(BF16)
    addr_out[:, 0, :] = 64.0 * mm_rows(named, high) + mm_rows(named, low)
    from_grid = mm_rows(chosen, mark(iota((grid_rows, edges), 0) == snd[...].reshape(1, edges))).astype(BF16)
    geo_rows = mm_rows(chosen, geo[...]).astype(BF16)

    loads[0].wait()
    loads[1].wait()
    hidden = silu(mm_cols(gf[...], gi[...])).astype(BF16)
    loads[2].wait()
    latent = norm_rows(mm(hidden, go[...])).astype(BF16)
    loads[3].wait()
    sender_proj = mm(latent, ee[0]).astype(BF16)
    grid_pick[...] = from_grid
    geo_pick[...] = geo_rows

    def fill(x):
        rows = pl.ds(x * (per * CAP), per * CAP)
        terms = mm(grid_pick[rows], sender_proj) + mm(geo_pick[rows], gw[...])
        outbox[pl.ds(x * per, per)] = terms.reshape(per, CAP, width).astype(BF16)

    fill(x0)
    pl.semaphore_wait(barrier, np_ + nb - 2)
    to_patches(addr_out, addr_in, 0, 0)
    to_column(outbox, inbox, 1, 19, 0)
    for dx in range(1, nx):
        fill((x0 + dx) % nx)
        to_column(outbox, inbox, 1, 19, dx)
    inbox[p] = outbox[p]

    loads[4].wait()
    recv_proj[...] = mm(mn[...], ee[1]).astype(BF16)
    loads[5].wait()
    loads[6].wait()
    edge_proj[...] = mm(me[...], pe[0])
    loads[7].wait()
    loads[8].wait()
    row = iota((padded, count), 0)
    own_pick = mark((iota((padded, count), 1) == b * share + row) & (row < share))
    own = mm(own_pick, mn[...]).astype(BF16)
    own_proj = mm(own, en[0])
    row, col = iota((padded, block), 0), iota((padded, block), 1)
    to_left = mark((row == col) & (row < share))
    to_right = mark(col == row + share)
    row, col = iota((block, padded), 0), iota((block, padded), 1)
    from_left = mark((row == col) & (row < share))
    from_right = mark(row == col + share)
    where_row = iota((wide, 1), 0).astype(F32)
    where_band = jnp.floor((where_row + 0.5) * (1.0 / block))
    within = where_row - block * where_band
    wide_node = where_band * share + jnp.where(within < share, within, within - share)
    left_rows = jnp.broadcast_to(within, (wide, half)) < share

    def in_halves(rows):
        picked = jnp.where(left_rows, rows[:, :half], rows[:, half:])
        return picked.reshape(nb, block, half).astype(BF16)

    def update(rows, rows_proj, arrived, weights):
        agg = arrived.astype(BF16)
        agg_left = mm(to_left, agg).astype(BF16)
        agg_right = mm(to_right, agg).astype(BF16)
        preact = rows_proj + mm(agg_left, weights[1, :half]) + mm(agg_right, weights[1, half:])
        return (rows.astype(F32) + tail(preact, weights[2])).astype(BF16)

    def packed(rows):
        return (mm(from_left, rows[:, :half]) + mm(from_right, rows[:, half:])).astype(BF16)

    row = iota((count, wide), 0).astype(F32)
    place = row + share * jnp.floor((row + 0.5) * (1.0 / share))
    col = iota((count, wide), 1).astype(F32)
    left_pick[...] = mark(col == place)
    right_pick[...] = mark(col == place + share)

    def natural(arrived, out):
        flat = arrived[...].astype(F32).reshape(wide, half).astype(BF16)
        out[:, :half] = mm(left_pick[...], flat).astype(BF16)
        out[:, half:] = mm(right_pick[...], flat).astype(BF16)

    settle(addr_in, rsem, 0)
    span = per * CAP
    placed[:, 0, :] = jnp.sum(addr_in[:, 0, :].reshape(nx, per, 128), axis=1)
    node_rows = iota((count, span), 0).astype(F32) + 1.0
    wide_rows = jnp.broadcast_to(wide_node + 1.0, (wide, span))
    for dx in range(nx):
        x = (x0 + nx - dx) % nx
        names = placed[x][:, :span]
        gathered = mm_cols(mark(node_rows == names), recv_proj[...])
        wide_landing = mark(wide_rows == names)
        wait_for(inbox.at[pl.ds(0, per - 1 if dx == 0 else per)], rsem.at[19 + dx])
        arrived = inbox[pl.ds(x * per, per)].astype(F32).reshape(span, width)
        message = tail(arrived + gathered, ee[2]).astype(BF16)
        landed = mm(wide_landing, message)
        if dx == 0:
            total[...] = landed
        elif dx < nx - 1:
            total[...] += landed
        else:
            rs_out[...] = in_halves(total[...] + landed)
    reduce_bands(rs_out, via_in, via_out, rs_in, 2, 7, 19 + nx)
    first = update(own, own_proj, reduced(rs_out, rs_in, 7), en)
    ag_out[...] = packed(first)
    gather_bands(ag_out, ag_in, 3, 10)
    relay_bands(ag_in, 3, 10)
    first_proj = mm(first, pn[0])

    spread_to = iota((np_ * 4, slots), 1)
    spread_from = iota((np_ * 4, slots), 0)
    spread = mark(spread_from == (spread_to >> 3) * 4 + (spread_to & 3))
    rows = jnp.broadcast_to(halo[...], (8, np_ * 4))
    wanted = 64.0 * mm((rows >> 6).astype(F32).astype(BF16), spread) + mm(
        (rows & 63).astype(F32).astype(BF16), spread
    )
    halo_pick = mark(iota((count, slots), 0).astype(F32) == wanted[0:1, :])
    left_slots = (iota((slots, half), 0) & 7) < 4
    local_pick = mark(iota((count, medges), 0) == msd[...])
    recv_pick = mark(iota((count, medges), 0) == mrc[...])
    ghost = msd[...] - count
    ghost_row = jnp.where(ghost < 0, -1024, (ghost >> 2) * 8 + (ghost & 3))
    ghost_left = mark(iota((slots, medges), 0) == ghost_row)
    ghost_right = mark(iota((slots, medges), 0) == ghost_row + 4)
    wide_recv = mark(
        jnp.broadcast_to(wide_node, (wide, medges)) == mrc[...].astype(F32)
    )

    wait_for(ag_in.at[pl.ds(0, 13)], rsem.at[12])
    natural(ag_in, one_ref)
    sent = mm(one_ref[...], pe[1]).astype(BF16)
    going = mm_cols(halo_pick, sent)
    going = jnp.where(left_slots, going[:, :half], going[:, half:])
    halo_out[...] = going.reshape(np_, CAP, half).astype(BF16)
    to_patches(halo_out, halo_in, 4, 4)
    recv_two = mm(one_ref[...], pe[2]).astype(BF16)
    edge_proj[...] += mm_cols(local_pick, sent) + mm_cols(recv_pick, recv_two)

    settle(halo_in, rsem, 4)
    ghosts = halo_in[...].astype(F32).reshape(slots, half).astype(BF16)
    edge_proj[:, :half] += mm_cols(ghost_left, ghosts)
    edge_proj[:, half:] += mm_cols(ghost_right, ghosts)
    edge_new = (me[...].astype(F32) + tail(edge_proj[...], pe[3])).astype(BF16)
    rs2_out[...] = in_halves(mm(wide_recv, edge_new))
    reduce_bands(rs2_out, via2_in, via2_out, rs2_in, 5, 13, 21 + nx)
    edge_ref[...] = edge_new
    second = update(first, first_proj, reduced(rs2_out, rs2_in, 13), pn)
    ag2_out[...] = packed(second)
    gather_bands(ag2_out, ag2_in, 6, 16)
    relay_bands(ag2_in, 6, 16)
    wait_for(ag2_in.at[pl.ds(0, 13)], rsem.at[18])
    natural(ag2_in, two_ref)

    settle(addr_in, ssem, 0)
    settle(inbox, ssem, 1)
    settle(rs_out, ssem, 2)
    settle(ag_in, ssem, 3)
    settle(halo_in, ssem, 4)
    settle(rs2_out, ssem, 5)
    settle(ag2_in, ssem, 6)


def per_device(
    nb, np_, ny,
    grid_feat, enc_sender, enc_patch, enc_node, enc_geo, mesh_nodes, mesh_edge, mesh_send,
    mesh_recv, halo_rows, grid_in, grid_out, geo_weight, enc_edge_w, enc_node_w, proc_edge_w,
    proc_node_w,
):
    edges = enc_sender.shape[0]
    count, width = mesh_nodes.shape
    medges = mesh_edge.shape[0]
    half = width // 2
    block = 2 * count // nb
    slots = np_ * CAP
    whole = pl.BlockSpec(memory_space=pltpu.VMEM)
    away = pl.BlockSpec(memory_space=pl.ANY)

    def like(v):
        return pltpu.VMEM(v.shape, v.dtype)

    return pl.pallas_call(
        functools.partial(kernel, nb, np_, ny),
        out_shape=(
            pltpu.VMEM((count, width), BF16),
            pltpu.VMEM((medges, width), BF16),
        ),
        in_specs=[away] * 3 + [whole] + [away] * 6 + [whole] * 7,
        out_specs=(whole, whole),
        scratch_shapes=[
            pltpu.VMEM(grid_feat.shape[::-1], BF16), like(grid_in), like(grid_out), like(enc_edge_w), like(enc_node_w),
            like(proc_edge_w), like(proc_node_w), like(mesh_nodes), like(mesh_edge),
            pltpu.SemaphoreType.DMA((9,)),
            pltpu.VMEM((np_, 1, 128), F32), pltpu.VMEM((np_, 1, 128), F32),
            pltpu.VMEM((np_, CAP, width), BF16), pltpu.VMEM((np_, CAP, width), BF16),
            pltpu.VMEM((nb, block, half), BF16), pltpu.VMEM((8, block, half), BF16),
            pltpu.VMEM((block, half), BF16), pltpu.VMEM((nb, block, half), BF16),
            pltpu.VMEM((np_, CAP, half), BF16), pltpu.VMEM((np_, CAP, half), BF16),
            pltpu.VMEM((nb, block, half), BF16), pltpu.VMEM((8, block, half), BF16),
            pltpu.VMEM((block, half), BF16), pltpu.VMEM((nb, block, half), BF16),
            pltpu.VMEM((7, block, half), BF16), pltpu.VMEM((2, block, half), BF16),
            pltpu.VMEM((7, block, half), BF16), pltpu.VMEM((2, block, half), BF16),
            pltpu.VMEM((count, 2 * count), BF16), pltpu.VMEM((count, 2 * count), BF16),
            pltpu.VMEM((count, width), BF16), pltpu.VMEM((medges, width), F32),
            pltpu.VMEM((count, width), BF16),
            pltpu.VMEM((np_ // (2 * ny), 1, 128), F32), pltpu.VMEM((2 * count, width), F32),
            pltpu.VMEM((slots, grid_feat.shape[0]), BF16), pltpu.VMEM((slots, 4), BF16),
            pltpu.SemaphoreType.DMA((7,)), pltpu.SemaphoreType.DMA((23 + np_ // (2 * ny),)),
        ],
        compiler_params=pltpu.CompilerParams(collective_id=0, has_side_effects=True),
    )(
        grid_feat.T, grid_in, grid_out, geo_weight, enc_edge_w, enc_node_w, proc_edge_w,
        proc_node_w, mesh_nodes, mesh_edge,
        enc_patch.reshape(1, edges), enc_sender, enc_node,
        enc_geo, mesh_send.reshape(1, medges), mesh_recv.reshape(1, medges), halo_rows,
    )


def solution(mesh):
    both = ("band", "patch")
    nb, np_ = mesh.shape["band"], mesh.shape["patch"]
    ny = 8 if np_ == 64 else np_ // 4
    placed = (
        P(both, None), P(both), P(both, None), P(both), P(None, both), P("patch", None),
        P(both, None), P(both), P(both), P("patch", None),
    ) + (P(),) * 7
    return jax.shard_map(
        functools.partial(per_device, nb, np_, ny),
        mesh=mesh,
        in_specs=placed,
        out_specs=(P("patch", None), P(both, None)),
        check_vma=False,
    )
```
